32 devices in a mesh: dp: 8 (over y, x, core), tensor: 4 (over z).
Axes of the slice: x: 2, y: 2, z: 4, core: 2. Of those that a mesh axis runs over, the one named last changes fastest.
Arguments:
- acts: bfloat16 [8192, 3584], P('dp'), may hold values from -6 to 6
- cotangent: bfloat16 [8192, 18944], P('dp', 'tensor'), may hold values from -6 to 6
- hessian_ema: float32 [3584, 18944], P('dp', 'tensor'), may hold values from 0.02 to 2
- momentum: float32 [3584, 18944], P('dp', 'tensor'), may hold values from -0.12 to 0.12
- gamma_table: float32 [28], replicated, may hold values from 0.005 to 0.02
- layer_index: int32 [1], replicated, may hold values from 0 to 27
- step_count: int32 [1], replicated, may hold values from 1 to 20
Outputs:
- new_hessian: float32 [67895296], P(('dp', 'tensor'))
- ratio: float32 [67895296], P(('dp', 'tensor'))
The draws below stay inside these ranges and needn't reach their ends.
All inputs are finite; a program needn't handle non-finite values.
Results may differ from the reference program's by a relative error of at most 0.0003.
Values sent between devices are 32-bit elements; how exact they have to be, the bound alone decides.
A program may use at most 192 MiB of HBM per device.

```python
import math
import jax
import jax.numpy as jnp
from jax import lax

D = 3584
FF = 18944
LAYERS_ALL = 28
TOKENS = 8192


def raised(array, rng, source, target, parts, factor):
    def block_of(axis_at):
        return (jnp.arange(array.shape[axis_at]) // (array.shape[axis_at] // parts)).reshape((-1,) + (1,) * (array.ndim - 1 - axis_at))

    one_side = jax.random.permutation(rng, parts)[block_of(target)]
    far = (block_of(target) + parts // 2) % parts
    return jnp.where((block_of(source) == one_side) | (block_of(source) == far), factor * array, array)


def block_scale(rng, shape, pieces, least, top_value):
    loudness = 1.0
    for axis_at, shards_of in pieces:
        draws = jax.random.uniform(jax.random.fold_in(jax.random.fold_in(rng, 6), axis_at), (shards_of,), jnp.float32, least / len(pieces), top_value / len(pieces))
        loudness = loudness * jnp.repeat(jnp.exp(draws), shape[axis_at] // shards_of).reshape((-1,) + (1,) * (len(shape) - 1 - axis_at))
    return loudness


def normal_values(own_key, dims, deviation, limit, shards=(), kind=jnp.bfloat16):
    array = deviation * jax.random.normal(own_key, dims, jnp.float32)
    if shards:
        array = array * block_scale(own_key, dims, shards, -0.22, 0.18)
    return jnp.clip(array, -limit, limit).astype(kind)


def gaussian_with(stream_key, extent, spread, reach, pieces, heavy, kind=jnp.bfloat16):
    values = spread * jax.random.normal(stream_key, extent, jnp.float32)
    if pieces:
        values = values * block_scale(stream_key, extent, pieces, -0.22, 0.18)
    return jnp.clip(raised(values, jax.random.fold_in(stream_key, 3), *heavy), -reach, reach).astype(kind)


def setup_inputs(seed: int = 0) -> dict:
    key_list = jax.random.split(jax.random.key(seed), 8)
    acts = gaussian_with(key_list[0], (TOKENS, D), 1.0, 6.0, ((0, 8),), (0, 1, 8, 2.0))
    cotangent = normal_values(key_list[1], (TOKENS, FF), 1.0, 6.0, ((0, 8), (1, 4)))
    hessian_ema = jnp.clip(jnp.exp(math.log(2.0) - 4.6051702 * jax.random.uniform(key_list[2], (D, FF), jnp.float32) ** block_scale(key_list[2], (D, FF), ((0, 8), (1, 4)), -0.2, 0.2)), 0.02, 2.0)
    momentum = normal_values(key_list[3], (D, FF), 0.02, 0.12, ((0, 8), (1, 4)), jnp.float32)
    gamma_table = jnp.clip(jnp.exp(jax.random.uniform(key_list[4], (LAYERS_ALL,), jnp.float32, math.log(0.005), math.log(0.02))), 0.005, 0.02)
    layer_index = jax.random.randint(key_list[5], (1,), 0, LAYERS_ALL).astype(jnp.int32)
    step_count = jax.random.randint(key_list[6], (1,), 1, 21).astype(jnp.int32)
    return {"acts": acts, "cotangent": cotangent, "hessian_ema": hessian_ema, "momentum": momentum, "gamma_table": gamma_table, "layer_index": layer_index, "step_count": step_count}


def reference(acts, cotangent, hessian_ema, momentum, gamma_table, layer_index, step_count):
    grad_sum = lax.dot_general(acts, cotangent, (((0,), (0,)), ((), ())), preferred_element_type=jnp.float32)
    estimate = grad_sum * grad_sum / float(TOKENS)
    fresh = 0.99 * hessian_ema + 0.01 * estimate
    picks = jnp.arange(LAYERS_ALL, dtype=jnp.int32) == layer_index[0]
    gamma = jnp.sum(jnp.where(picks, gamma_table, jnp.zeros_like(gamma_table)))
    correction = 1.0 - jnp.power(jnp.asarray(0.99, gamma_table.dtype), step_count[0].astype(gamma_table.dtype))
    corrected = fresh / correction
    ratio = jnp.clip(momentum / (gamma * corrected), -1.0, 1.0)
    return fresh.reshape(-1), ratio.reshape(-1)
```

```python
import jax
import jax.numpy as jnp
from jax import lax
from jax.sharding import PartitionSpec as P

SHARES = (2, 2, 2, 1)
EARLY = 2


def settle(grad_part, hess_part, mom_part, tokens_all, gamma, correction):
    estimate = grad_part * grad_part / tokens_all
    fresh = 0.99 * hess_part + 0.01 * estimate
    corrected = fresh / correction
    ratio = jnp.clip(mom_part / (gamma * corrected), -1.0, 1.0)
    return (fresh, ratio)


def swap(block):
    return lax.all_to_all(block, "tensor", split_axis=0, concat_axis=1, tiled=True)


def cuts_of(rows):
    unit = next(u for u in (16, 8, 4, 2, 1) if rows % u == 0)
    units, total, edges, upto = rows // unit, sum(SHARES), [0], 0
    for share in SHARES:
        upto += share
        edges.append(unit * (units * upto // total))
    return list(zip(edges, edges[1:]))


def on_device(acts, cotangent, hessian_ema, momentum, gamma_table, layer_index, step_count):
    dp = lax.axis_size("dp")
    tensor = lax.axis_size("tensor")
    tokens_all = float(acts.shape[0] * dp)
    picks = jnp.arange(gamma_table.shape[0], dtype=jnp.int32) == layer_index[0]
    gamma = jnp.sum(jnp.where(picks, gamma_table, jnp.zeros_like(gamma_table)))
    correction = 1.0 - jnp.power(
        jnp.asarray(0.99, gamma_table.dtype), step_count[0].astype(gamma_table.dtype)
    )
    width = cotangent.shape[1]
    rows = hessian_ema.shape[0] // tensor
    whole = tensor * width
    acts_rows = acts.T.reshape(dp * tensor, rows, acts.shape[0])
    hess_rows = hessian_ema.reshape(tensor, rows, width)
    mom_rows = momentum.reshape(tensor, rows, width)
    cuts = cuts_of(rows)

    def block(states, a, b):
        return states[:, a:b].reshape(tensor * (b - a), width)

    partials = []
    for a, b in cuts:
        partial = lax.dot_general(
            acts_rows[:, a:b].reshape(dp * tensor * (b - a), acts.shape[0]),
            cotangent,
            (((1,), (0,)), ((), ())),
            preferred_element_type=jnp.float32,
        )
        partial, acts_rows = lax.optimization_barrier((partial, acts_rows))
        partials.append(partial)
    sums = [lax.psum_scatter(p, "dp", scatter_dimension=0, tiled=True) for p in partials]
    late = cuts[EARLY][0]
    moved_hess = swap(block(hess_rows, late, rows))
    moved_mom = swap(block(mom_rows, late, rows))
    sums[0], moved_hess, moved_mom = lax.optimization_barrier(
        (sums[0], moved_hess, moved_mom) + tuple(p[:8, :128] for p in partials[1:])
    )[:3]

    fresh_all = jnp.zeros((rows * whole,), jnp.float32)
    ratio_all = jnp.zeros((rows * whole,), jnp.float32)
    for step, (a, b) in enumerate(cuts):
        if step < EARLY:
            fresh, ratio = settle(
                sums[step], block(hess_rows, a, b), block(mom_rows, a, b), tokens_all, gamma, correction
            )
            fresh, ratio = swap(fresh), swap(ratio)
            if step + 1 < len(cuts):
                sums[step + 1], fresh, ratio = lax.optimization_barrier((sums[step + 1], fresh, ratio))
        else:
            fresh, ratio = settle(
                swap(sums[step]),
                moved_hess[a - late : b - late],
                moved_mom[a - late : b - late],
                tokens_all,
                gamma,
                correction,
            )
        fresh_all = lax.dynamic_update_slice(fresh_all, fresh.reshape(-1), (a * whole,))
        ratio_all = lax.dynamic_update_slice(ratio_all, ratio.reshape(-1), (a * whole,))
    return (fresh_all, ratio_all)


def solution(mesh):
    placed = (P("dp", None), P("dp", "tensor"), P("dp", "tensor"), P("dp", "tensor"), P(), P(), P())
    return jax.shard_map(
        on_device,
        mesh=mesh,
        in_specs=placed,
        out_specs=(P(("dp", "tensor")), P(("dp", "tensor"))),
        check_vma=False,
    )
```
